128 devices in a mesh: dp: 16 (over x, z_hi, core), fsdp: 8 (over z_lo, y).
Axes of the slice: x: 4, y: 4, z: 4 (z_hi: 2, z_lo: 2; z = z_hi * 2 + z_lo), core: 2. Of those that a mesh axis runs over, the one named last changes fastest.
Arguments:
- activations: bfloat16 [98304, 8192], P(('dp', 'fsdp')), may hold values from -6 to 6
- out_grad: bfloat16 [98304, 1024], P(('dp', 'fsdp')), may hold values from -24 to 24
- master: float32 [1024, 8192], P('fsdp', 'dp'), may hold values from -0.0625 to 0.0625
- moment1: float32 [1024, 8192], P('fsdp', 'dp'), may hold values from -6 to 6
- moment2: float32 [1024, 8192], P('fsdp', 'dp'), may hold values from 0.2 to 5
Outputs:
- new_weight: bfloat16 [1024, 8192], P('fsdp')
- master_out: float32 [1024, 8192], P('fsdp', 'dp')
- moment1_out: float32 [1024, 8192], P('fsdp', 'dp')
- moment2_out: float32 [1024, 8192], P('fsdp', 'dp')
The draws below stay inside these ranges and needn't reach their ends.
All inputs are finite; a program needn't handle non-finite values.
Results may differ from the reference program's by a relative error of at most 0.005.
Values may be sent and summed in bfloat16 or wider, within the bound.
No kernel may reach another device: no remote copies, remote signals or barrier semaphores. Data moves between devices by JAX's collectives and lax.ppermute only.
A program may use at most 128 MiB of HBM per device.

```python
import math
import jax
import jax.numpy as jnp
from jax import lax

D = 8192
STEP = 3
TOK_DEV = 768
F = 1024
TOKENS = 98304
N_DP = 16
N_FSDP = 8


def with_spikes(values, stream_key, source, target, shards_of, factor):
    owner, partner = [(jnp.arange(values.shape[dim]) // (values.shape[dim] // shards_of)).reshape([-1 if axis == dim else 1 for axis in range(values.ndim)]) for dim in (source, target)]
    chosen = jax.random.permutation(stream_key, shards_of)[partner]
    strong = (owner == chosen) | (owner == (partner + shards_of // 2) % shards_of)
    return jnp.where(strong, factor * values, values)


def steps_of(stream_key, extent, split, low, high):
    loudness, own = 1.0, jax.random.fold_in(stream_key, 6)
    for dim, shards_of in split:
        draws = jnp.exp(jax.random.uniform(jax.random.fold_in(own, dim), (shards_of,), jnp.float32, low / len(split), high / len(split)))
        loudness = loudness * jnp.repeat(draws, extent[dim] // shards_of).reshape([-1 if axis == dim else 1 for axis in range(len(extent))])
    return loudness


def centred(stream_key, extent, spread, most, shards=(), dtype=jnp.bfloat16):
    drawn = spread * jax.random.normal(stream_key, extent, jnp.float32)
    if shards:
        drawn = drawn * steps_of(stream_key, extent, shards, -0.22, 0.18)
    return jnp.clip(drawn, -most, most).astype(dtype)


def bell_draw_with(stream_key, dims, width, reach, cuts, heavy, held_as=jnp.bfloat16):
    entries = width * jax.random.normal(stream_key, dims, jnp.float32)
    if cuts:
        entries = entries * steps_of(stream_key, dims, cuts, -0.22, 0.18)
    return jnp.clip(with_spikes(entries, jax.random.fold_in(stream_key, 3), *heavy), -reach, reach).astype(held_as)


def setup_inputs(seed: int = 0) -> dict:
    key_of = jax.random.split(jax.random.key(seed), 6)
    return {
        "activations": centred(key_of[0], (TOKENS, D), 1.0, 6.0, ((0, 128),)),
        "out_grad": bell_draw_with(key_of[1], (TOKENS, F), 1.0, 24.0, ((0, 128),), (0, 1, 128, 5.5)),
        "master": centred(key_of[2], (F, D), D ** -0.5, 0.0625, ((0, 8), (1, 16)), jnp.float32),
        "moment1": centred(key_of[3], (F, D), 1.0, 6.0, ((0, 8), (1, 16)), jnp.float32),
        "moment2": jnp.clip(jnp.exp(math.log(5.0) - 3.218876 * jax.random.uniform(key_of[4], (F, D), jnp.float32) ** steps_of(key_of[4], (F, D), ((0, 8), (1, 16)), -0.2, 0.2)), 0.2, 5.0),
    }


def reference(activations, out_grad, master, moment1, moment2):
    total_tokens = activations.shape[0]
    scale = float(total_tokens) ** (-0.5)

    def accumulate(index, total):
        start = (index * TOK_DEV).astype(jnp.int32)
        inputs = lax.dynamic_slice_in_dim(activations, start, TOK_DEV, 0)
        upstream = lax.dynamic_slice_in_dim(out_grad, start, TOK_DEV, 0)
        partial_value = jnp.dot(upstream.T, inputs, preferred_element_type=jnp.float32) * scale
        rounded = lax.optimization_barrier(partial_value.astype(jnp.bfloat16))
        return total + rounded.astype(jnp.float32)
    empty = jnp.zeros((out_grad.shape[1], activations.shape[1]), jnp.float32)
    grad = lax.fori_loop(0, N_DP * N_FSDP, accumulate, empty)
    moment1_out = 0.9 * moment1 + 0.1 * grad
    moment2_out = 0.95 * moment2 + 0.05 * grad * grad
    first_fix = 1.0 - 0.9 ** STEP
    second_fix = 1.0 - 0.95 ** STEP
    update = moment1_out / first_fix / (jnp.sqrt(moment2_out / second_fix) + 1e-08)
    master_out = master - 0.01 * (update + 0.1 * master)
    new_weight = master_out.astype(jnp.bfloat16)
    return (new_weight, master_out, moment1_out, moment2_out)
```

```python
import functools
import itertools

import jax
import jax.numpy as jnp
from jax import lax
from jax.experimental import pallas as pl
from jax.experimental.pallas import tpu as pltpu
from jax.sharding import PartitionSpec as P

STEP = 3
AXES = ("dp", "fsdp")
ROWS_A = 96
ROWS_C = 32
HOPS = [(dx, dz) for dx in (0, 1, 3, 2) for dz in (0, 2)]


def place(x, z, c, y):
    x, z, y = x % 4, z % 4, y % 4
    return ((x * 2 + z // 2) * 2 + c) * 8 + (z % 2) * 4 + y


def moved(step):
    pairs = []
    for x, z, c, y in itertools.product(range(4), range(4), range(2), range(4)):
        dx, dz, dc, dy = step(c)
        pairs.append((place(x, z, c, y), place(x + dx, z + dz, c ^ dc, y + dy)))
    return pairs


def send(value, step):
    return lax.ppermute(value, AXES, moved(step))


def swap_cores(value):
    return send(value, lambda c: (0, 0, 1, 0))


def along_first(d):
    return lambda c: (d, 0, 0, 0) if c == 0 else (0, 0, 0, d)


def along_second(d):
    return lambda c: (0, 0, 0, d) if c == 0 else (d, 0, 0, 0)


def along_z(d):
    return lambda c: (0, d, 0, 0)


def product_kernel(scale, half_ref, grad_ref, first_ref, second_ref, a_ref, c_ref, a_buf, c_buf, sems):
    step = pl.program_id(0)
    slot = step % 2
    first = half_ref[0] == 0

    def each(step, slot, act):
        for y in range(4):
            target = a_ref.at[jnp.where(first, step, y), jnp.where(first, y, step)]
            act(pltpu.make_async_copy(a_buf.at[slot, y], target, sems.at[slot, y]))
        for z in range(4):

            @pl.when(first)
            def _():
                act(pltpu.make_async_copy(c_buf.at[slot, z], c_ref.at[z, :, step], sems.at[slot, 4 + z]))

            @pl.when(jnp.logical_not(first))
            def _():
                act(pltpu.make_async_copy(c_buf.at[slot, z], c_ref.at[z, step], sems.at[slot, 4 + z]))

    @pl.when(step >= 2)
    def _():
        each(step - 2, slot, lambda copy: copy.wait())

    for i, act_ref in enumerate((first_ref, second_ref)):
        value = lax.dot_general(
            grad_ref[...], act_ref[...], (((0,), (0,)), ((), ())), preferred_element_type=jnp.float32
        )
        value = (value * scale).astype(jnp.bfloat16).reshape(2, 4, 128, 512)
        for low in range(2):
            for y in range(4):
                a_buf[slot, y, 2 * i + low] = value[low, y, :ROWS_A]
                c_buf[slot, 2 * i + low, y] = value[low, y, ROWS_A:]
    each(step, slot, lambda copy: copy.start())

    @pl.when(step == 3)
    def _():
        each(step - 1, 1 - slot, lambda copy: copy.wait())
        each(step, slot, lambda copy: copy.wait())


def products(half, out_grad, act, scale):
    tokens = act.shape[0]
    shapes = [(4, 4, 4, r, 512) for r in (ROWS_A, ROWS_C)]
    return pl.pallas_call(
        functools.partial(product_kernel, scale),
        grid_spec=pltpu.PrefetchScalarGridSpec(
            num_scalar_prefetch=1,
            grid=(4,),
            in_specs=[
                pl.BlockSpec((tokens, 1024), lambda k, h: (0, 0)),
                pl.BlockSpec((tokens, 512), lambda k, h: (0, 4 * k + h[0])),
                pl.BlockSpec((tokens, 512), lambda k, h: (0, 4 * k + 2 + h[0])),
            ],
            out_specs=[pl.BlockSpec(memory_space=pl.ANY)] * 2,
            scratch_shapes=[pltpu.VMEM((2, *s[1:]), jnp.bfloat16) for s in shapes]
            + [pltpu.SemaphoreType.DMA((2, 8))],
        ),
        out_shape=[jax.ShapeDtypeStruct(s, jnp.bfloat16) for s in shapes],
        compiler_params=pltpu.CompilerParams(dimension_semantics=("arbitrary",)),
        cost_estimate=pl.CostEstimate(
            flops=2 * 1024 * tokens * 4096, bytes_accessed=tokens * 8192, transcendentals=0
        ),
    )(half, out_grad, act, act)


def fold_kernel(one_ref, z_ref, two_ref, *refs):
    a_refs, c_refs, out_refs = refs[:5], refs[5:10], refs[10:]

    def write(out_ref):
        for group, start, stop in ((a_refs, 0, ROWS_A), (c_refs, ROWS_A, 128)):
            for i in range(4):
                for row in range(0, stop - start, 16):
                    cut = (i, pl.ds(row, 16))
                    pieces = [ref[(0,) * (len(ref.shape) - 3) + cut] for ref in group]
                    out_ref[i, pl.ds(start + row, 16)] = total(pieces).astype(jnp.bfloat16)

    for j, out_ref in enumerate(out_refs):

        @pl.when(pl.program_id(0) == j)
        def _():
            write(out_ref)


def fold(one, z, two, a_parts, c_parts):
    in_specs = []
    for k, rows in enumerate((ROWS_A, ROWS_C)):
        whole = pl.BlockSpec(
            (1, 1, 4, rows, 512), lambda j, *w, k=k: (w[k][0], (w[2][0] + j + 1) % 4, 0, 0, 0)
        )
        part = pl.BlockSpec((1, 4, rows, 512), lambda j, *w: ((w[2][0] + j + 1) % 4, 0, 0, 0))
        in_specs += [whole, whole, part, part, part]
    return pl.pallas_call(
        fold_kernel,
        grid_spec=pltpu.PrefetchScalarGridSpec(
            num_scalar_prefetch=3,
            grid=(4,),
            in_specs=in_specs,
            out_specs=[pl.BlockSpec((4, 128, 512), lambda j, *w: (0, 0, 0))] * 4,
        ),
        out_shape=[jax.ShapeDtypeStruct((4, 128, 512), jnp.bfloat16)] * 4,
        compiler_params=pltpu.CompilerParams(dimension_semantics=("arbitrary",)),
        cost_estimate=pl.CostEstimate(flops=2**24, bytes_accessed=2**23, transcendentals=0),
    )(one, z, two, *a_parts, *c_parts)


def assemble_kernel(dp_ref, own_ref, other_ref, out_ref, sems):
    dp = dp_ref[0]
    x, zh, c = dp >> 2, (dp >> 1) & 1, dp & 1
    copies = []
    for i, (dx, dz) in enumerate(HOPS):
        base = ((x + 4 - dx) & 3) * 4 + (zh ^ (dz // 2)) * 2
        for j, ref in enumerate((own_ref, other_ref)):
            start = pl.multiple_of((base + (c ^ j)) * 512, 512)
            copies.append(
                pltpu.make_async_copy(ref.at[i], out_ref.at[:, pl.ds(start, 512)], sems.at[2 * i + j])
            )
    for copy in copies:
        copy.start()
    for copy in copies:
        copy.wait()


def assemble(dp, own, other):
    return pl.pallas_call(
        assemble_kernel,
        in_specs=[
            pl.BlockSpec(memory_space=pltpu.SMEM),
            pl.BlockSpec(memory_space=pltpu.VMEM),
            pl.BlockSpec(memory_space=pltpu.VMEM),
        ],
        out_specs=pl.BlockSpec(memory_space=pl.ANY),
        out_shape=jax.ShapeDtypeStruct((128, 8192), jnp.bfloat16),
        scratch_shapes=[pltpu.SemaphoreType.DMA((16,))],
        compiler_params=pltpu.CompilerParams(vmem_limit_bytes=8 * 2**20),
    )(dp, own, other)


def at(value, index, dim):
    return lax.dynamic_index_in_dim(value, index, dim, keepdims=False)


def scalar(value):
    return value.reshape(1).astype(jnp.int32)


def total(pieces):
    return functools.reduce(lambda a, b: a + b, [p.astype(jnp.float32) for p in pieces])


def body(activations, out_grad, master, moment1, moment2):
    scale = float(activations.shape[0] * 128) ** (-0.5)
    dp, fsdp = lax.axis_index("dp"), lax.axis_index("fsdp")
    x, zh, c = dp // 4, dp // 2 % 2, dp % 2
    zl, y = fsdp // 4, fsdp % 4
    z = zh * 2 + zl
    first = c == 0
    one, two = jnp.where(first, x, y), jnp.where(first, y, x)


    sent_a, sent_c = products(scalar(1 - c), out_grad, activations, scale)
    got_a, got_c = swap_cores(sent_a), swap_cores(sent_c)
    own_a, own_c = products(scalar(c), out_grad, activations, scale)

    steps = (1, 2, 3)

    def exchange(pair, place, step):
        parts = [total([at(v, (place + d) % 4, 0) for v in pair]).astype(jnp.bfloat16) for d in steps]
        return [*pair, *(send(p, step(d)) for p, d in zip(parts, steps))]

    a1 = exchange((own_a, got_a), one, along_first)
    c1 = exchange((own_c, got_c), z, along_z)
    parts = fold(scalar(one), scalar(z), scalar(two), a1, c1)
    both = total([send(p, along_second(d)) for p, d in zip(parts, steps)] + [parts[3]])
    both = both.astype(jnp.bfloat16)
    a2, c2 = both[:, :ROWS_A], both[:, ROWS_A:]
    a3 = total([at(a2, z, 0)] + [send(at(a2, (z + d) % 4, 0), along_z(d)) for d in steps])
    c3 = total([at(c2, one, 0)] + [send(at(c2, (one + d) % 4, 0), along_first(d)) for d in steps])
    grad = jnp.concatenate([a3, c3], axis=0)

    moment1_out = 0.9 * moment1 + 0.1 * grad
    moment2_out = 0.95 * moment2 + 0.05 * grad * grad
    first_fix = 1.0 - 0.9**STEP
    second_fix = 1.0 - 0.95**STEP
    update = moment1_out / first_fix / (jnp.sqrt(moment2_out / second_fix) + 1e-08)
    master_out = master - 0.01 * (update + 0.1 * master)
    weight = master_out.astype(jnp.bfloat16)

    own = jnp.stack(
        [weight if h == (0, 0) else send(weight, lambda c, h=h: (h[0], h[1], 0, 0)) for h in HOPS]
    )
    new_weight = assemble(scalar(dp), own, swap_cores(own))
    return (new_weight, master_out, moment1_out, moment2_out)


def solution(mesh):
    in_specs = (P(AXES, None), P(AXES, None), P("fsdp", "dp"), P("fsdp", "dp"), P("fsdp", "dp"))
    out_specs = (P("fsdp", None), P("fsdp", "dp"), P("fsdp", "dp"), P("fsdp", "dp"))
    return jax.shard_map(body, mesh=mesh, in_specs=in_specs, out_specs=out_specs, check_vma=False)
```

```python
import functools
import itertools

import jax
import jax.numpy as jnp
from jax import lax
from jax.experimental import pallas as pl
from jax.experimental.pallas import tpu as pltpu
from jax.sharding import PartitionSpec as P


STEP = 3
AXES = ("dp", "fsdp")


def place(x, z, c, y):
    x, z, y = x % 4, z % 4, y % 4
    return ((x * 2 + z // 2) * 2 + c) * 8 + (z % 2) * 4 + y


def moved(step):
    pairs = []
    for x, z, c, y in itertools.product(range(4), range(4), range(2), range(4)):
        dx, dz, dc, dy = step(c)
        pairs.append((place(x, z, c, y), place(x + dx, z + dz, c ^ dc, y + dy)))
    return pairs


def send(value, step):
    return lax.ppermute(value, AXES, moved(step))


def swap_cores(value):
    return send(value, lambda c: (0, 0, 1, 0))


def along_first(d):
    return lambda c: (d, 0, 0, 0) if c == 0 else (0, 0, 0, d)


def along_second(d):
    return lambda c: (0, 0, 0, d) if c == 0 else (d, 0, 0, 0)


def along_z(d):
    return lambda c: (0, d, 0, 0)


def product_kernel(scale, place_ref, grad_ref, first_ref, second_ref, far_ref, rest_ref, buf, sems):
    step = pl.program_id(0)
    slot = step % 2
    first = place_ref[0] == 0

    def each(step, slot, act):
        for y in range(4):
            one, other = jnp.where(first, step, y), jnp.where(first, y, step)
            hops = (one - place_ref[1]) & 3

            @pl.when(hops == 2)
            def _():
                act(pltpu.make_async_copy(buf.at[slot, y], far_ref.at[other], sems.at[slot, y]))

            @pl.when(hops != 2)
            def _():
                target = rest_ref.at[jnp.where(hops == 0, 2, hops >> 1), other]
                act(pltpu.make_async_copy(buf.at[slot, y], target, sems.at[slot, y]))

    @pl.when(step >= 2)
    def _():
        each(step - 2, slot, lambda copy: copy.wait())

    for i, act_ref in enumerate((first_ref, second_ref)):
        value = lax.dot_general(
            grad_ref[...], act_ref[...], (((0,), (0,)), ((), ())), preferred_element_type=jnp.float32
        )
        value = (value * scale).astype(jnp.bfloat16).reshape(2, 4, 128, 512)
        for low in range(2):
            for y in range(4):
                buf[slot, y, 2 * i + low] = value[low, y]
    each(step, slot, lambda copy: copy.start())

    @pl.when(step == 3)
    def _():
        each(step - 1, 1 - slot, lambda copy: copy.wait())
        each(step, slot, lambda copy: copy.wait())


def products(place, out_grad, act, scale):
    tokens = act.shape[0]
    shapes = [(4, 4, 128, 512), (3, 4, 4, 128, 512)]
    return pl.pallas_call(
        functools.partial(product_kernel, scale),
        grid_spec=pltpu.PrefetchScalarGridSpec(
            num_scalar_prefetch=1,
            grid=(4,),
            in_specs=[
                pl.BlockSpec((tokens, 1024), lambda k, h: (0, 0)),
                pl.BlockSpec((tokens, 512), lambda k, h: (0, 4 * k + h[0])),
                pl.BlockSpec((tokens, 512), lambda k, h: (0, 4 * k + 2 + h[0])),
            ],
            out_specs=[pl.BlockSpec(memory_space=pl.ANY)] * 2,
            scratch_shapes=[
                pltpu.VMEM((2, 4, 4, 128, 512), jnp.bfloat16),
                pltpu.SemaphoreType.DMA((2, 4)),
            ],
        ),
        out_shape=[jax.ShapeDtypeStruct(s, jnp.bfloat16) for s in shapes],
        compiler_params=pltpu.CompilerParams(dimension_semantics=("arbitrary",)),
        cost_estimate=pl.CostEstimate(
            flops=2 * 1024 * tokens * 4096, bytes_accessed=tokens * 8192, transcendentals=0
        ),
    )(place, out_grad, act, act)


def fold_kernel(two_ref, keep_ref, *refs):
    low_refs, high_refs, out_refs = refs[:2], refs[2:4], refs[4:]
    pieces = ((2, 0, 2), (2, 2, 2), (1, 0, 2), (3, 2, 2), (1, 2, 2), (3, 0, 2), (0, 0, 4))
    for (hops, start, count), out_ref in zip(pieces, out_refs):
        turn = (two_ref[0] + hops) & 3

        def write(refs, local, out_ref=out_ref, start=start, count=count, turn=turn):
            def rows(n, carry):
                i, row = n // 4, pl.multiple_of(n % 4 * 32, 32)
                cut = pl.ds(row, 32)
                values = [keep_ref[turn, start + i, cut]] + [r[local, start + i, cut] for r in refs]
                out_ref[i, cut] = total(values).astype(jnp.bfloat16)
                return carry

            lax.fori_loop(0, 4 * count, rows, 0)

        @pl.when(turn < 2)
        def _():
            write(low_refs, turn)

        @pl.when(turn >= 2)
        def _():
            write(high_refs, turn - 2)


def fold(two, keep, low, high):
    counts = (2, 2, 2, 2, 2, 2, 4)
    return pl.pallas_call(
        fold_kernel,
        in_specs=[pl.BlockSpec(memory_space=pltpu.SMEM)]
        + [pl.BlockSpec(memory_space=pltpu.VMEM)] * 5,
        out_specs=[pl.BlockSpec(memory_space=pltpu.VMEM)] * 7,
        out_shape=[jax.ShapeDtypeStruct((n, 128, 512), jnp.bfloat16) for n in counts],
        compiler_params=pltpu.CompilerParams(vmem_limit_bytes=16 * 2**20),
        cost_estimate=pl.CostEstimate(flops=2**24, bytes_accessed=2**23, transcendentals=0),
    )(two, keep, *low, *high)


def assemble_kernel(dp_ref, *refs):
    ins, out_ref, sems = refs[:9], refs[9], refs[10]
    dp = dp_ref[0]
    x, zh, c = dp >> 2, (dp >> 1) & 1, dp & 1
    copies = []

    def place(piece, x, zh, c):
        start = pl.multiple_of(((x & 3) * 4 + zh * 2 + c) * 512, 512)
        n = len(copies)
        copies.append(pltpu.make_async_copy(piece, out_ref.at[:, pl.ds(start, 512)], sems.at[n]))

    for i in range(2):
        place(ins[0].at[i], x, zh, c ^ i)
        for owner, held in ((c, ins[1:5]), (1 - c, ins[5:9])):
            side = x + 3 + 2 * owner
            place(held[0].at[i], side, zh, owner ^ i)
            place(held[1].at[i], side, 1 - zh, owner ^ i)
            place(held[2].at[i], x + 2, zh ^ owner, owner ^ i)
            if i == 0:
                place(held[3], x, 1 - zh, owner)
    for copy in copies:
        copy.start()
    for copy in copies:
        copy.wait()


def assemble(dp, *pieces):
    return pl.pallas_call(
        assemble_kernel,
        in_specs=[pl.BlockSpec(memory_space=pltpu.SMEM)]
        + [pl.BlockSpec(memory_space=pltpu.VMEM)] * 9,
        out_specs=pl.BlockSpec(memory_space=pl.ANY),
        out_shape=jax.ShapeDtypeStruct((128, 8192), jnp.bfloat16),
        scratch_shapes=[pltpu.SemaphoreType.DMA((16,))],
        compiler_params=pltpu.CompilerParams(vmem_limit_bytes=8 * 2**20),
    )(dp, *pieces)


def gathered(dp, weight):
    over = send(weight, lambda c: (0, 2, 0, 0))
    both = jnp.stack([weight, swap_cores(weight)])
    held = [
        send(both, lambda c: (1 - 2 * c, 0, 0, 0)),
        send(both, lambda c: (1 - 2 * c, 2, 0, 0)),
        send(both, lambda c: (2, 2 * c, 0, 0)),
        over,
    ]
    return assemble(dp, both, *held, *(swap_cores(v) for v in held))


def at(value, index, dim):
    return lax.dynamic_index_in_dim(value, index, dim, keepdims=False)


def scalars(*values):
    return jnp.stack(values).astype(jnp.int32)


def total(pieces):
    return functools.reduce(lambda a, b: a + b, [p.astype(jnp.float32) for p in pieces])


def step_of(activations, out_grad, master, moment1, moment2):
    scale = float(activations.shape[0] * 128) ** (-0.5)
    dp, fsdp = lax.axis_index("dp"), lax.axis_index("fsdp")
    x, zh, c = dp // 4, dp // 2 % 2, dp % 2
    zl, y = fsdp // 4, fsdp % 4
    z = zh * 2 + zl
    first = c == 0
    one, two = jnp.where(first, x, y), jnp.where(first, y, x)


    def added(*values):
        return total(values).astype(jnp.bfloat16)

    sent_far, sent_rest = products(scalars(1 - c, two), out_grad, activations, scale)
    got_far, got_rest = swap_cores(sent_far), swap_cores(sent_rest)
    own_far, own_rest = products(scalars(c, one), out_grad, activations, scale)

    far_low, far_high = added(own_far[:2], got_far[:2]), added(own_far[2:], got_far[2:])
    low, high = send(far_low, along_first(3)), send(far_high, along_first(1))
    (own_rest, got_rest), _ = lax.optimization_barrier(((own_rest, got_rest), (far_low, far_high)))
    up_low = added(own_rest[0, :2], got_rest[0, :2])
    down_high = added(own_rest[1, 2:], got_rest[1, 2:])
    (own_rest, got_rest), _ = lax.optimization_barrier(((own_rest, got_rest), (up_low, down_high)))
    up_high = added(own_rest[0, 2:], got_rest[0, 2:], high)
    down_low = added(own_rest[1, :2], got_rest[1, :2], low)
    keep = lax.optimization_barrier(added(own_rest[2], got_rest[2]))
    up_low, down_high = send(up_low, along_first(1)), send(down_high, along_first(3))
    lows = up_low, send(down_low, along_first(3))
    highs = send(up_high, along_first(1)), down_high
    far_low, far_high, up_low, down_high, up_high, down_low, keep = fold(scalars(two), keep, lows, highs)

    decayed1, decayed2 = lax.optimization_barrier((0.9 * moment1, 0.95 * moment2))
    low, high = send(far_low, along_second(3)), send(far_high, along_second(1))
    up_low, down_high = send(up_low, along_second(1)), send(down_high, along_second(3))
    up_high = send(added(up_high, high), along_second(1))
    down_low = send(added(down_low, low), along_second(3))
    sums = jnp.concatenate([added(keep[:2], up_low, down_low), added(keep[2:], up_high, down_high)])

    grad = total([at(sums, z, 0)] + [send(at(sums, (z + d) % 4, 0), along_z(d)) for d in (1, 3, 2)])

    moment1_out = decayed1 + 0.1 * grad
    moment2_out = decayed2 + 0.05 * grad * grad
    first_fix = 1.0 - 0.9**STEP
    second_fix = 1.0 - 0.95**STEP
    update = moment1_out / first_fix / (jnp.sqrt(moment2_out / second_fix) + 1e-08)
    master_out = master - 0.01 * (update + 0.1 * master)
    weight = master_out.astype(jnp.bfloat16)

    new_weight = gathered(scalars(dp), weight)
    return (new_weight, master_out, moment1_out, moment2_out)


def solution(mesh):
    in_specs = (P(AXES, None), P(AXES, None), P("fsdp", "dp"), P("fsdp", "dp"), P("fsdp", "dp"))
    out_specs = (P("fsdp", None), P("fsdp", "dp"), P("fsdp", "dp"), P("fsdp", "dp"))
    return jax.shard_map(step_of, mesh=mesh, in_specs=in_specs, out_specs=out_specs, check_vma=False)
```

```python
import functools
import itertools

import jax
import jax.numpy as jnp
from jax import lax
from jax.experimental import pallas as pl
from jax.experimental.pallas import tpu as pltpu
from jax.sharding import PartitionSpec as P


STEP = 3
AXES = ("dp", "fsdp")


def place(x, z, c, y):
    x, z, y = x % 4, z % 4, y % 4
    return ((x * 2 + z // 2) * 2 + c) * 8 + (z % 2) * 4 + y


def moved(step):
    pairs = []
    for x, z, c, y in itertools.product(range(4), range(4), range(2), range(4)):
        dx, dz, dc, dy = step(c)
        pairs.append((place(x, z, c, y), place(x + dx, z + dz, c ^ dc, y + dy)))
    return pairs


def send(value, step):
    return lax.ppermute(value, AXES, moved(step))


def swap_cores(value):
    return send(value, lambda c: (0, 0, 1, 0))


def along_first(d):
    return lambda c: (d, 0, 0, 0) if c == 0 else (0, 0, 0, d)


def along_second(d):
    return lambda c: (0, 0, 0, d) if c == 0 else (d, 0, 0, 0)


def along_z(d):
    return lambda c: (0, d, 0, 0)


def product_kernel(scale, place_ref, grad_ref, first_ref, second_ref, far_ref, rest_ref):
    step = pl.program_id(0)
    first = place_ref[0] == 0
    for i, act_ref in enumerate((first_ref, second_ref)):
        value = lax.dot_general(
            grad_ref[...], act_ref[...], (((0,), (0,)), ((), ())), preferred_element_type=jnp.float32
        )
        value = (value * scale).astype(jnp.bfloat16).reshape(2, 4, 128, 512)
        for y in range(4):
            one, other = jnp.where(first, step, y), jnp.where(first, y, step)
            hops = (one - place_ref[1]) & 3

            @pl.when(hops == 2)
            def _():
                for low in range(2):
                    far_ref[other, 2 * i + low] = value[low, y]

            @pl.when(hops != 2)
            def _():
                for low in range(2):
                    rest_ref[jnp.where(hops == 0, 2, hops >> 1), other, 2 * i + low] = value[low, y]


def products(place, out_grad, act, scale):
    tokens = act.shape[0]
    shapes = [(4, 4, 128, 512), (3, 4, 4, 128, 512)]
    return pl.pallas_call(
        functools.partial(product_kernel, scale),
        grid_spec=pltpu.PrefetchScalarGridSpec(
            num_scalar_prefetch=1,
            grid=(4,),
            in_specs=[
                pl.BlockSpec((tokens, 1024), lambda k, h: (0, 0)),
                pl.BlockSpec((tokens, 512), lambda k, h: (0, 4 * k + h[0])),
                pl.BlockSpec((tokens, 512), lambda k, h: (0, 4 * k + 2 + h[0])),
            ],
            out_specs=[pl.BlockSpec(memory_space=pltpu.VMEM)] * 2,
        ),
        out_shape=[pltpu.VMEM(s, jnp.bfloat16) for s in shapes],
        compiler_params=pltpu.CompilerParams(
            dimension_semantics=("arbitrary",), vmem_limit_bytes=28 * 2**20
        ),
        cost_estimate=pl.CostEstimate(
            flops=2 * 1024 * tokens * 4096, bytes_accessed=tokens * 8192, transcendentals=0
        ),
    )(place, out_grad, *[pltpu.with_memory_space_constraint(act, pltpu.HBM)] * 2)


def fold_kernel(two_ref, keep_ref, *refs):
    low_refs, high_refs, out_refs = refs[:2], refs[2:4], refs[4:]
    pieces = ((2, 0, 2), (2, 2, 2), (1, 0, 2), (3, 2, 2), (1, 2, 2), (3, 0, 2), (0, 0, 4))
    for (hops, start, count), out_ref in zip(pieces, out_refs):
        turn = (two_ref[0] + hops) & 3

        def write(refs, local, out_ref=out_ref, start=start, count=count, turn=turn):
            def rows(n, carry):
                i, row = n // 4, pl.multiple_of(n % 4 * 32, 32)
                cut = pl.ds(row, 32)
                values = [keep_ref[turn, start + i, cut]] + [r[local, start + i, cut] for r in refs]
                out_ref[i, cut] = total(values).astype(jnp.bfloat16)
                return carry

            lax.fori_loop(0, 4 * count, rows, 0)

        @pl.when(turn < 2)
        def _():
            write(low_refs, turn)

        @pl.when(turn >= 2)
        def _():
            write(high_refs, turn - 2)


def fold(two, keep, low, high):
    counts = (2, 2, 2, 2, 2, 2, 4)
    return pl.pallas_call(
        fold_kernel,
        in_specs=[pl.BlockSpec(memory_space=pltpu.SMEM)]
        + [pl.BlockSpec(memory_space=pltpu.VMEM)] * 5,
        out_specs=[pl.BlockSpec(memory_space=pltpu.VMEM)] * 7,
        out_shape=[jax.ShapeDtypeStruct((n, 128, 512), jnp.bfloat16) for n in counts],
        compiler_params=pltpu.CompilerParams(vmem_limit_bytes=16 * 2**20),
        cost_estimate=pl.CostEstimate(flops=2**24, bytes_accessed=2**23, transcendentals=0),
    )(two, keep, *low, *high)


def assemble_kernel(dp_ref, *refs):
    ins, out_ref, sems = refs[:9], refs[9], refs[10]
    dp = dp_ref[0]
    x, zh, c = dp >> 2, (dp >> 1) & 1, dp & 1
    copies = []

    def place(piece, x, zh, c):
        start = pl.multiple_of(((x & 3) * 4 + zh * 2 + c) * 512, 512)
        n = len(copies)
        copies.append(pltpu.make_async_copy(piece, out_ref.at[:, pl.ds(start, 512)], sems.at[n]))

    for i in range(2):
        place(ins[0].at[i], x, zh, c ^ i)
        for owner, held in ((c, ins[1:5]), (1 - c, ins[5:9])):
            side = x + 3 + 2 * owner
            place(held[0].at[i], side, zh ^ owner, owner ^ i)
            place(held[1].at[i], side, 1 - (zh ^ owner), owner ^ i)
            place(held[2].at[i], x + 2, zh ^ owner, owner ^ i)
            if i == 0:
                place(held[3], x, 1 - zh, owner)
    for copy in copies:
        copy.start()
    for copy in copies:
        copy.wait()


def assemble(dp, *pieces):
    return pl.pallas_call(
        assemble_kernel,
        in_specs=[pl.BlockSpec(memory_space=pltpu.SMEM)]
        + [pl.BlockSpec(memory_space=pltpu.VMEM)] * 9,
        out_specs=pl.BlockSpec(memory_space=pl.ANY),
        out_shape=jax.ShapeDtypeStruct((128, 8192), jnp.bfloat16),
        scratch_shapes=[pltpu.SemaphoreType.DMA((16,))],
        compiler_params=pltpu.CompilerParams(vmem_limit_bytes=8 * 2**20),
    )(dp, *pieces)


def gathered(dp, weight):
    over = send(weight, lambda c: (0, 2, 0, 0))
    both = jnp.stack([weight, swap_cores(weight)])
    near = send(both, lambda c: (1 - 2 * c, 2 * c, 0, 0))
    held = [
        near,
        send(both, lambda c: (1 - 2 * c, 2 - 2 * c, 0, 0)),
        send(near, lambda c: (1 - 2 * c, 0, 0, 0)),
        over,
    ]
    return assemble(dp, both, *held, *(swap_cores(v) for v in held))


def at(value, index, dim):
    return lax.dynamic_index_in_dim(value, index, dim, keepdims=False)


def scalars(*values):
    return jnp.stack(values).astype(jnp.int32)


def total(pieces):
    return functools.reduce(lambda a, b: a + b, [p.astype(jnp.float32) for p in pieces])


def step_of(activations, out_grad, master, moment1, moment2):
    scale = float(activations.shape[0] * 128) ** (-0.5)
    dp, fsdp = lax.axis_index("dp"), lax.axis_index("fsdp")
    x, zh, c = dp // 4, dp // 2 % 2, dp % 2
    zl, y = fsdp // 4, fsdp % 4
    z = zh * 2 + zl
    first = c == 0
    one, two = jnp.where(first, x, y), jnp.where(first, y, x)


    def added(*values):
        return total(values).astype(jnp.bfloat16)

    sent_far, sent_rest = products(scalars(1 - c, two), out_grad, activations, scale)
    got_far, got_rest = swap_cores(sent_far), swap_cores(sent_rest)
    own_far, own_rest = products(scalars(c, one), out_grad, activations, scale)

    far_low, far_high = added(own_far[:2], got_far[:2]), added(own_far[2:], got_far[2:])
    low, high = send(far_low, along_first(3)), send(far_high, along_first(1))
    (own_rest, got_rest), _ = lax.optimization_barrier(((own_rest, got_rest), (far_low, far_high)))
    up_low = added(own_rest[0, :2], got_rest[0, :2])
    down_high = added(own_rest[1, 2:], got_rest[1, 2:])
    (own_rest, got_rest), _ = lax.optimization_barrier(((own_rest, got_rest), (up_low, down_high)))
    up_high = added(own_rest[0, 2:], got_rest[0, 2:], high)
    down_low = added(own_rest[1, :2], got_rest[1, :2], low)
    keep = lax.optimization_barrier(added(own_rest[2], got_rest[2]))
    up_low, down_high = send(up_low, along_first(1)), send(down_high, along_first(3))
    lows = up_low, send(down_low, along_first(3))
    highs = send(up_high, along_first(1)), down_high
    far_low, far_high, up_low, down_high, up_high, down_low, keep = fold(scalars(two), keep, lows, highs)

    decayed1, decayed2 = lax.optimization_barrier((0.9 * moment1, 0.95 * moment2))
    low, high = send(far_low, along_second(3)), send(far_high, along_second(1))
    up_low, down_high = send(up_low, along_second(1)), send(down_high, along_second(3))
    up_high = send(added(up_high, high), along_second(1))
    down_low = send(added(down_low, low), along_second(3))
    sums = jnp.concatenate([added(keep[:2], up_low, down_low), added(keep[2:], up_high, down_high)])

    grad = total([at(sums, z, 0)] + [send(at(sums, (z + d) % 4, 0), along_z(d)) for d in (1, 3, 2)])

    moment1_out = decayed1 + 0.1 * grad
    moment2_out = decayed2 + 0.05 * grad * grad
    first_fix = 1.0 - 0.9**STEP
    second_fix = 1.0 - 0.95**STEP
    update = moment1_out / first_fix / (jnp.sqrt(moment2_out / second_fix) + 1e-08)
    master_out = master - 0.01 * (update + 0.1 * master)
    weight = master_out.astype(jnp.bfloat16)

    new_weight = gathered(scalars(dp), weight)
    return (new_weight, master_out, moment1_out, moment2_out)


def solution(mesh):
    in_specs = (P(AXES, None), P(AXES, None), P("fsdp", "dp"), P("fsdp", "dp"), P("fsdp", "dp"))
    out_specs = (P("fsdp", None), P("fsdp", "dp"), P("fsdp", "dp"), P("fsdp", "dp"))
    return jax.shard_map(step_of, mesh=mesh, in_specs=in_specs, out_specs=out_specs, check_vma=False)
```
